32 devices in a mesh: rep: 2 (over y), blk: 8 (over z, x), head: 2 (over core).
Axes of the slice: x: 2, y: 2, z: 4, core: 2. Of those that a mesh axis runs over, the one named last changes fastest.
Arguments:
- queries: bfloat16 [2, 512, 8192], P('rep', 'blk', 'head'), parts along dimension 0, may hold values from -200 to 200
- keys: bfloat16 [2, 512, 512], P('rep', 'blk', 'head'), parts along dimension 0, may hold values from -6 to 6
- values: bfloat16 [2, 512, 512], P('rep', 'blk', 'head'), parts along dimension 0, may hold values from -6 to 6
- prompt_length: int32 [2], P('rep'), parts along dimension 0, may hold values from 256 to 512
- span_order: int32 [32], P('rep'), parts along dimension 0, may hold values from 0 to 15, as said below
Outputs:
- attended: bfloat16 [2, 512, 8192], P('rep', 'blk', 'head'), parts along dimension 0
The draws below stay inside these ranges and needn't reach their ends.
There are 2 independent parts, one for each index of `rep`. The reference program is written for one: setup_inputs(seed, part) draws one part's arguments, and reference() takes and returns one part's arrays. A program takes and returns all parts, laid end to end along the dimension named above; each array names one. Nothing has to cross between parts.
Inputs may be any that keep to these rules, and one draw needn't show every extreme that they name: `span_order`: each of the 16 span numbers stands in exactly one slot.
All inputs are finite; a program needn't handle non-finite values.
Results may differ from the reference program's by a relative error of at most 0.0065.
Values may be sent and summed in bfloat16 or wider, within the bound.
A program may use at most 64 MiB of HBM per device.

```python
import jax
import jax.numpy as jnp
from jax import lax

CH = 32
REPLICA_PROMPTS = 1
KEY_VALUE_HEADS = 4
QUERY_PER_KV = 16
HEAD_WIDTH = 128
NCHUNK = 16
PROMPT_TOKENS = 512


def span_table(key):
    return jax.random.permutation(jax.random.fold_in(key, 11), NCHUNK).astype(jnp.int32)


def draw_span_order(key, part):
    return span_table(key)


def base_keys(key):
    unscaled_scores = jax.random.normal(jax.random.fold_in(key, 23), (REPLICA_PROMPTS, PROMPT_TOKENS, KEY_VALUE_HEADS, HEAD_WIDTH), jnp.float32)
    return jnp.clip(unscaled_scores, -6.0, 6.0)


def draw_keys(key, part):
    unscaled_scores = base_keys(key)
    return unscaled_scores.reshape(REPLICA_PROMPTS, PROMPT_TOKENS, KEY_VALUE_HEADS * HEAD_WIDTH).astype(jnp.bfloat16)


def draw_queries(key, part):
    unscaled_scores = jax.random.normal(jax.random.fold_in(key, 31), (REPLICA_PROMPTS, PROMPT_TOKENS, KEY_VALUE_HEADS, QUERY_PER_KV, HEAD_WIDTH), jnp.float32)
    unscaled_scores = jnp.clip(unscaled_scores, -6.0, 6.0)
    return unscaled_scores.reshape(REPLICA_PROMPTS, PROMPT_TOKENS, KEY_VALUE_HEADS * QUERY_PER_KV * HEAD_WIDTH).astype(jnp.bfloat16)


def block_levels(key, dims, cuts, low, high):
    gain, own = 1.0, jax.random.fold_in(key, 6)
    for dim, shards_of in cuts:
        draws = jnp.exp(jax.random.uniform(jax.random.fold_in(own, dim), (shards_of,), jnp.float32, low / len(cuts), high / len(cuts)))
        gain = gain * jnp.repeat(draws, dims[dim] // shards_of).reshape([-1 if axis == dim else 1 for axis in range(len(dims))])
    return gain


def normal_values(key, shape, width, bound, pieces=(), held_as=jnp.bfloat16):
    entries = jax.random.normal(key, shape, jnp.float32) * width
    if len(pieces) > 0:
        entries = block_levels(key, shape, pieces, -0.22, 0.18) * entries
    return jnp.clip(entries, min=-bound, max=bound).astype(held_as)


def setup_inputs(seed: int = 0, part: int = 0) -> dict:
    key_list = jax.random.split(jax.random.key(seed), 6)
    part_splits = jax.random.split(jax.random.fold_in(key_list[5], part), 6)
    queries = draw_queries(jax.random.fold_in(jax.random.fold_in(key_list[5], part), 71), part)
    keys = draw_keys(jax.random.fold_in(jax.random.fold_in(key_list[5], part), 71), part)
    values = normal_values(part_splits[2], (REPLICA_PROMPTS, PROMPT_TOKENS, KEY_VALUE_HEADS * HEAD_WIDTH), 1.0, 6.0, ((1, 8), (2, 2)))
    prompt_length = jax.random.randint(part_splits[3], (REPLICA_PROMPTS,), PROMPT_TOKENS // 2, PROMPT_TOKENS + 1).astype(jnp.int32)
    span_order = draw_span_order(jax.random.fold_in(jax.random.fold_in(key_list[5], part), 71), part)
    return {"queries": queries, "keys": keys, "values": values, "prompt_length": prompt_length, "span_order": span_order}


NEG_FILL = -1e30


def one_prompt(queries, keys, values, limit, position):
    allowed = (position[None, :] <= position[:, None]) & (position[None, :] < limit)
    query_heads = queries.reshape(PROMPT_TOKENS, KEY_VALUE_HEADS, QUERY_PER_KV, HEAD_WIDTH).transpose(1, 2, 0, 3).reshape(KEY_VALUE_HEADS * QUERY_PER_KV, PROMPT_TOKENS, HEAD_WIDTH)
    key_heads = jnp.repeat(keys.reshape(PROMPT_TOKENS, KEY_VALUE_HEADS, HEAD_WIDTH).transpose(1, 0, 2), QUERY_PER_KV, axis=0)
    value_heads = jnp.repeat(values.reshape(PROMPT_TOKENS, KEY_VALUE_HEADS, HEAD_WIDTH).transpose(1, 0, 2), QUERY_PER_KV, axis=0)
    scale = HEAD_WIDTH ** -0.5

    def one_head(parts):
        query, key_rows, value_rows = parts
        scores = jnp.dot(query, key_rows.T, preferred_element_type=jnp.float32) * scale
        scores = jnp.where(allowed, scores, NEG_FILL)
        top = jnp.max(scores, axis=1, keepdims=True)
        weights = jnp.where(allowed, jnp.exp(scores - top), 0.0)
        total = jnp.sum(weights, axis=1, keepdims=True)
        mixed = jnp.dot(weights.astype(jnp.bfloat16), value_rows, preferred_element_type=jnp.float32)
        return mixed / total

    head_results = lax.map(one_head, (query_heads, key_heads, value_heads))
    joined_heads = head_results.reshape(KEY_VALUE_HEADS, QUERY_PER_KV, PROMPT_TOKENS, HEAD_WIDTH).transpose(2, 0, 1, 3).reshape(PROMPT_TOKENS, KEY_VALUE_HEADS * QUERY_PER_KV * HEAD_WIDTH)
    joined_heads = jnp.where((position < limit)[:, None], joined_heads, 0.0)
    return joined_heads.astype(jnp.bfloat16)


def reference(queries, keys, values, prompt_length, span_order):
    offsets = jnp.arange(CH, dtype=jnp.int32)
    position = (span_order[:, None].astype(jnp.int32) * CH + offsets[None, :]).reshape(-1).astype(jnp.int32)
    outputs = []
    for index in range(REPLICA_PROMPTS):
        outputs.append(one_prompt(queries[index], keys[index], values[index], prompt_length[index], position))
    return jnp.stack(outputs)
```

```python
import functools
import math

import jax
import jax.numpy as jnp
from jax import lax
from jax.experimental import pallas as pl
from jax.experimental.pallas import tpu as pltpu
from jax.sharding import PartitionSpec as P

HEAD_WIDTH = 128
NEG_FILL = -1e30
HEADS_PER_TILE = 4
KEY_CHUNK = 512
MESH = pl.DeviceIdType.MESH


def kernel(
    blocks, local_heads, group, spans, q_hbm, k_hbm, v_hbm, len_ref, order_ref, o_ref,
    q_ref, k_ref, v_ref, bias_ref, q_sem, own_sem, send_sem, recv_sem
):
    rows = q_ref.shape[0]
    span = rows // spans
    keys = blocks * rows
    me = lax.axis_index("blk")
    own = pl.ds(me * rows, rows)
    q_copy = pltpu.make_async_copy(q_hbm.at[0], q_ref, q_sem)
    k_copy = pltpu.make_async_copy(k_hbm.at[0], k_ref.at[own], own_sem.at[0])
    v_copy = pltpu.make_async_copy(v_hbm.at[0], v_ref.at[own], own_sem.at[1])
    k_copy.start()
    v_copy.start()
    q_copy.start()

    barrier = pltpu.get_barrier_semaphore()
    for d in range(1, blocks):
        pl.semaphore_signal(
            barrier, inc=1, device_id={"blk": lax.rem(me + d, blocks)}, device_id_type=MESH
        )
    pl.semaphore_wait(barrier, blocks - 1)

    def send(ref, which, d):
        return pltpu.make_async_remote_copy(
            src_ref=ref.at[own],
            dst_ref=ref.at[own],
            send_sem=send_sem.at[which, d - 1],
            recv_sem=recv_sem.at[which, d - 1],
            device_id={"blk": lax.rem(me + d, blocks)},
            device_id_type=MESH,
        )

    def arrival(ref, which, d):
        source = lax.rem(me + blocks - d, blocks)
        there = pl.ds(source * rows, rows)
        return pltpu.make_async_remote_copy(
            src_ref=ref.at[there],
            dst_ref=ref.at[there],
            send_sem=send_sem.at[which, d - 1],
            recv_sem=recv_sem.at[which, d - 1],
            device_id={"blk": lax.rem(me + d, blocks)},
            device_id_type=MESH,
        )

    k_copy.wait()
    for d in range(1, blocks):
        send(k_ref, 0, d).start()
    v_copy.wait()
    for d in range(1, blocks):
        send(v_ref, 1, d).start()

    limit = len_ref[0]
    row = lax.broadcasted_iota(jnp.int32, (rows, 1), 0)
    row_pos = jnp.zeros((rows, 1), jnp.int32)
    for t in range(spans):
        row_pos = jnp.where(row // span == t, order_ref[me * spans + t] * span + row % span, row_pos)
    chunk = min(keys, KEY_CHUNK)
    chunks = keys // chunk
    lane = lax.broadcasted_iota(jnp.int32, (1, chunk), 1)

    def make_bias(c):
        key_pos = jnp.zeros((1, chunk), jnp.int32)
        for t in range(chunk // span):
            key_pos = jnp.where(
                lane // span == t, order_ref[c * (chunk // span) + t] * span + lane % span, key_pos
            )
        allowed = (key_pos <= row_pos) & (key_pos < limit)
        bias_ref[c] = jnp.where(allowed, 0.0, NEG_FILL)

    pl.loop(0, chunks)(make_bias)
    live = row_pos < limit
    q_copy.wait()

    for which, ref in ((0, k_ref), (1, v_ref)):
        for d in range(1, blocks):
            arrival(ref, which, d).wait_recv()

    scale = HEAD_WIDTH ** (-0.5) * math.log2(math.e)
    tile = HEADS_PER_TILE if group % HEADS_PER_TILE == 0 else 1
    height = tile * rows
    ones = jnp.ones((chunk, HEAD_WIDTH), jnp.bfloat16)

    for h in range(local_heads):
        cols = slice(h * HEAD_WIDTH, (h + 1) * HEAD_WIDTH)

        def run_tile(i, h=h, cols=cols):
            first = h * group * HEAD_WIDTH + i * (tile * HEAD_WIDTH)

            def q_cols(t):
                return pl.ds(pl.multiple_of(first + t * HEAD_WIDTH, HEAD_WIDTH), HEAD_WIDTH)

            q = jnp.concatenate([q_ref[:, q_cols(t)] for t in range(tile)], axis=0)

            def part(c):
                at = pl.ds(pl.multiple_of(c * chunk, chunk), chunk)
                score = lax.dot_general(
                    q, k_ref[at, cols], (((1,), (1,)), ((), ())), preferred_element_type=jnp.float32
                )
                score = (score * scale).reshape(tile, rows, chunk) + bias_ref[c][None]
                return score.reshape(height, chunk), jnp.concatenate([v_ref[at, cols], ones], axis=1)

            if chunks == 1:
                score, value = part(0)
                top = jnp.max(score, axis=1, keepdims=True)
                weight = jnp.exp2(score - top).astype(jnp.bfloat16)
                mixed = jnp.dot(weight, value, preferred_element_type=jnp.float32)
            else:

                def step(c, state):
                    best, mixed = state
                    score, value = part(c)
                    top = jnp.maximum(best, jnp.max(score, axis=1, keepdims=True))
                    weight = jnp.exp2(score - top).astype(jnp.bfloat16)
                    fresh = jnp.dot(weight, value, preferred_element_type=jnp.float32)
                    return top, mixed * jnp.exp2(best - top) + fresh

                init = (
                    jnp.full((height, 1), NEG_FILL, jnp.float32),
                    jnp.zeros((height, 2 * HEAD_WIDTH), jnp.float32),
                )
                _, mixed = lax.fori_loop(0, chunks, step, init)
            out = mixed[:, :HEAD_WIDTH] / mixed[:, HEAD_WIDTH:]
            for t in range(tile):
                piece = jnp.where(live, out[t * rows : (t + 1) * rows], 0.0)
                o_ref[0, :, q_cols(t)] = piece.astype(o_ref.dtype)

        pl.loop(0, group // tile)(run_tile)

    for which, ref in ((0, k_ref), (1, v_ref)):
        for d in range(1, blocks):
            send(ref, which, d).wait_send()


def solution(mesh):
    blocks = mesh.shape["blk"]

    def shards(queries, keys, values, prompt_length, span_order):
        _, rows, width = queries.shape
        kv_width = keys.shape[2]
        local_heads = kv_width // HEAD_WIDTH
        group = width // kv_width
        total = blocks * rows
        chunk = min(total, KEY_CHUNK)
        anywhere = pl.BlockSpec(memory_space=pl.ANY)
        scalars = pl.BlockSpec(memory_space=pltpu.SMEM)
        return pl.pallas_call(
            functools.partial(kernel, blocks, local_heads, group, span_order.shape[0] // blocks),
            out_shape=jax.ShapeDtypeStruct(queries.shape, queries.dtype),
            in_specs=[anywhere, anywhere, anywhere, scalars, scalars],
            out_specs=pl.BlockSpec(memory_space=pltpu.VMEM),
            scratch_shapes=[
                pltpu.VMEM((rows, width), queries.dtype),
                pltpu.VMEM((total, kv_width), keys.dtype),
                pltpu.VMEM((total, kv_width), values.dtype),
                pltpu.VMEM((total // chunk, rows, chunk), jnp.float32),
                pltpu.SemaphoreType.DMA,
                pltpu.SemaphoreType.DMA((2,)),
                pltpu.SemaphoreType.DMA((2, blocks - 1)),
                pltpu.SemaphoreType.DMA((2, blocks - 1)),
            ],
            compiler_params=pltpu.CompilerParams(
                collective_id=0, has_side_effects=True, vmem_limit_bytes=56 * 1024 * 1024
            ),
        )(queries, keys, values, prompt_length, span_order)

    spec = P("rep", "blk", "head")
    return jax.shard_map(
        shards, mesh=mesh, in_specs=(spec, spec, spec, P("rep"), P("rep")), out_specs=spec, check_vma=False
    )
```

```python
import functools
import math

import jax
import jax.numpy as jnp
from jax import lax
from jax.experimental import pallas as pl
from jax.experimental.pallas import tpu as pltpu
from jax.sharding import PartitionSpec as P

HEAD_WIDTH = 128
NEG_FILL = -1e30
HEADS_PER_TILE = 2
KEY_CHUNK = 512
MESH = pl.DeviceIdType.MESH


def row_length(blocks):
    return max(d for d in range(1, math.isqrt(blocks) + 1) if blocks % d == 0)


def kernel(
    rows_z, cols_x, local_heads, group, spans, q_hbm, k_hbm, v_hbm, len_ref, order_ref, o_ref,
    q_ref, k_ref, v_ref, bias_ref, q_sem, own_sem,
    col_send, col_recv, row_send, row_recv
):
    blocks = rows_z * cols_x
    rows = q_ref.shape[0]
    span = rows // spans
    keys = blocks * rows
    me = lax.axis_index("blk")
    own = pl.ds(me * rows, rows)
    q_copy = pltpu.make_async_copy(q_hbm.at[0], q_ref, q_sem)
    k_copy = pltpu.make_async_copy(k_hbm.at[0], k_ref.at[own], own_sem.at[0])
    v_copy = pltpu.make_async_copy(v_hbm.at[0], v_ref.at[own], own_sem.at[1])
    k_copy.start()
    v_copy.start()
    q_copy.start()

    z, x = lax.div(me, cols_x), lax.rem(me, cols_x)
    refs = (k_ref, v_ref)

    def block(row, col):
        return pl.ds((row * cols_x + col) * rows, rows)

    def wrapped(row):
        return lax.rem(row + rows_z, rows_z)

    def peer(e):
        return z * cols_x + lax.rem(x + e, cols_x)

    def copy(u, at, target, send, recv):
        return pltpu.make_async_remote_copy(
            src_ref=refs[u].at[at],
            dst_ref=refs[u].at[at],
            send_sem=send,
            recv_sem=recv,
            device_id={"blk": target},
            device_id_type=MESH,
        )

    def to_column(row, u):
        return copy(u, own, row * cols_x + x, col_send.at[row, u], col_recv.at[z, u])

    def from_column(row, u):
        return copy(u, block(row, x), row * cols_x + x, col_send.at[row, u], col_recv.at[row, u])

    def to_row(row, e, u):
        return copy(u, block(row, x), peer(e), row_send.at[row, e - 1, u], row_recv.at[row, e - 1, u])

    def from_row(row, e, u):
        col = lax.rem(x + cols_x - e, cols_x)
        return copy(u, block(row, col), peer(e), row_send.at[row, e - 1, u], row_recv.at[row, e - 1, u])

    def each_row(distances, visit):
        for d in distances:
            pl.when(z + d < rows_z)(lambda d=d: visit(z + d))
            pl.when(z >= d)(lambda d=d: visit(z - d))

    near = range(1, rows_z)
    send_order = tuple(reversed(near))
    barrier = pltpu.get_barrier_semaphore()

    def greet(target):
        pl.semaphore_signal(barrier, inc=1, device_id={"blk": target}, device_id_type=MESH)

    for d in near:
        greet(lax.rem(me + d * cols_x, blocks))
    for e in range(1, cols_x):
        greet(peer(e))
    pl.semaphore_wait(barrier, rows_z + cols_x - 2)

    for u, own_copy in enumerate((k_copy, v_copy)):
        own_copy.wait()
        each_row(send_order, lambda row, u=u: to_column(row, u).start())
        for e in range(1, cols_x):
            to_row(z, e, u).start()

    def relay(row, u):
        from_column(row, u).wait_recv()
        for e in range(1, cols_x):
            to_row(row, e, u).start()

    def gather_row(row, u):
        for e in range(1, cols_x):
            from_row(row, e, u).wait_recv()

    def drain():
        for u in range(2):
            for d in near:
                to_column(lax.rem(z + d, rows_z), u).wait_send()
            for row in range(rows_z):
                for e in range(1, cols_x):
                    to_row(row, e, u).wait_send()

    limit = len_ref[0]
    row = lax.broadcasted_iota(jnp.int32, (rows, 1), 0)
    row_pos = jnp.zeros((rows, 1), jnp.int32)
    for t in range(spans):
        row_pos = jnp.where(row // span == t, order_ref[me * spans + t] * span + row % span, row_pos)
    chunk = min(keys, KEY_CHUNK)
    chunks = keys // chunk
    lane = lax.broadcasted_iota(jnp.int32, (1, chunk), 1)

    def make_bias(c):
        key_pos = jnp.zeros((1, chunk), jnp.int32)
        for t in range(chunk // span):
            key_pos = jnp.where(
                lane // span == t, order_ref[c * (chunk // span) + t] * span + lane % span, key_pos
            )
        allowed = (key_pos <= row_pos) & (key_pos < limit)
        bias_ref[c] = jnp.where(allowed, 0.0, NEG_FILL)

    pl.loop(0, chunks)(make_bias)
    live = row_pos < limit
    q_copy.wait()

    for u in range(2):
        each_row(tuple(reversed(near)), lambda row, u=u: relay(row, u))
    for u in range(2):
        for row in range(rows_z):
            gather_row(row, u)

    scale = HEAD_WIDTH ** (-0.5) * math.log2(math.e)
    tile = HEADS_PER_TILE if group % HEADS_PER_TILE == 0 else 1
    height = tile * rows
    ones = jnp.ones((chunk, HEAD_WIDTH), jnp.bfloat16)

    for h in range(local_heads):
        cols = slice(h * HEAD_WIDTH, (h + 1) * HEAD_WIDTH)

        def run_tile(i, h=h, cols=cols):
            first = h * group * HEAD_WIDTH + i * (tile * HEAD_WIDTH)

            def q_cols(t):
                return pl.ds(pl.multiple_of(first + t * HEAD_WIDTH, HEAD_WIDTH), HEAD_WIDTH)

            q = jnp.concatenate([q_ref[:, q_cols(t)] for t in range(tile)], axis=0)

            def part(c):
                at = pl.ds(pl.multiple_of(c * chunk, chunk), chunk)
                score = lax.dot_general(
                    q, k_ref[at, cols], (((1,), (1,)), ((), ())), preferred_element_type=jnp.float32
                )
                score = (score * scale).reshape(tile, rows, chunk) + bias_ref[c][None]
                return score.reshape(height, chunk), jnp.concatenate([v_ref[at, cols], ones], axis=1)

            if chunks == 1:
                score, value = part(0)
                top = jnp.max(score, axis=1, keepdims=True)
                weight = jnp.exp2(score - top).astype(jnp.bfloat16)
                mixed = jnp.dot(weight, value, preferred_element_type=jnp.float32)
            else:

                def step(c, state):
                    best, mixed = state
                    score, value = part(c)
                    top = jnp.maximum(best, jnp.max(score, axis=1, keepdims=True))
                    weight = jnp.exp2(score - top).astype(jnp.bfloat16)
                    fresh = jnp.dot(weight, value, preferred_element_type=jnp.float32)
                    return top, mixed * jnp.exp2(best - top) + fresh

                init = (
                    jnp.full((height, 1), NEG_FILL, jnp.float32),
                    jnp.zeros((height, 2 * HEAD_WIDTH), jnp.float32),
                )
                _, mixed = lax.fori_loop(0, chunks, step, init)
            out = mixed[:, :HEAD_WIDTH] / mixed[:, HEAD_WIDTH:]
            for t in range(tile):
                piece = jnp.where(live, out[t * rows : (t + 1) * rows], 0.0)
                o_ref[0, :, q_cols(t)] = piece.astype(o_ref.dtype)

        pl.loop(0, group // tile, unroll=True)(run_tile)

    drain()


def solution(mesh):
    blocks = mesh.shape["blk"]
    cols_x = row_length(blocks)
    rows_z = blocks // cols_x

    def shards(queries, keys, values, prompt_length, span_order):
        _, rows, width = queries.shape
        kv_width = keys.shape[2]
        local_heads = kv_width // HEAD_WIDTH
        group = width // kv_width
        total = blocks * rows
        chunk = min(total, KEY_CHUNK)
        held = rows * width * 2 + total * kv_width * 4 + total * rows * 4
        anywhere = pl.BlockSpec(memory_space=pl.ANY)
        scalars = pl.BlockSpec(memory_space=pltpu.SMEM)
        return pl.pallas_call(
            functools.partial(kernel, rows_z, cols_x, local_heads, group, span_order.shape[0] // blocks),
            out_shape=jax.ShapeDtypeStruct(queries.shape, queries.dtype),
            in_specs=[anywhere, anywhere, anywhere, scalars, scalars],
            out_specs=pl.BlockSpec(memory_space=pltpu.VMEM),
            scratch_shapes=[
                pltpu.VMEM((rows, width), queries.dtype),
                pltpu.VMEM((total, kv_width), keys.dtype),
                pltpu.VMEM((total, kv_width), values.dtype),
                pltpu.VMEM((total // chunk, rows, chunk), jnp.float32),
                pltpu.SemaphoreType.DMA,
                pltpu.SemaphoreType.DMA((2,)),
                *[pltpu.SemaphoreType.DMA((rows_z, 2))] * 2,
                *[pltpu.SemaphoreType.DMA((rows_z, cols_x, 2))] * 2,
            ],
            compiler_params=pltpu.CompilerParams(
                collective_id=0, has_side_effects=True, vmem_limit_bytes=held + 6 * 1024 * 1024
            ),
        )(queries, keys, values, prompt_length, span_order)

    spec = P("rep", "blk", "head")
    return jax.shard_map(
        shards, mesh=mesh, in_specs=(spec, spec, spec, P("rep"), P("rep")), out_specs=spec, check_vma=False
    )
```

```python
import functools
import math

import jax
import jax.numpy as jnp
from jax import lax
from jax.experimental import pallas as pl
from jax.experimental.pallas import tpu as pltpu
from jax.sharding import PartitionSpec as P

HEAD_WIDTH = 128
NEG_FILL = -1e30
HEADS_PER_TILE = 2
KEY_CHUNK = 512
OUT_PARTS = 2
VMEM_LIMIT = 56 * 1024 * 1024
MESH = pl.DeviceIdType.MESH


def row_length(blocks):
    return max(d for d in range(1, math.isqrt(blocks) + 1) if blocks % d == 0)


def kernel(
    rows_z, cols_x, local_heads, group, spans, q_hbm, k_hbm, v_hbm, len_hbm, order_hbm, o_hbm,
    q_ref, o_ref, k_ref, v_ref, bias_ref, len_ref, order_ref, q_sem, own_sem, small_sem, out_sem,
    col_send, col_recv, row_send, row_recv
):
    blocks = rows_z * cols_x
    rows = q_ref.shape[0]
    span = rows // spans
    keys = blocks * rows
    me = lax.axis_index("blk")
    own = pl.ds(me * rows, rows)
    q_copy = pltpu.make_async_copy(q_hbm.at[0], q_ref, q_sem)
    k_copy = pltpu.make_async_copy(k_hbm.at[0], k_ref.at[own], own_sem.at[0])
    v_copy = pltpu.make_async_copy(v_hbm.at[0], v_ref.at[own], own_sem.at[1])
    k_copy.start()
    v_copy.start()
    q_copy.start()
    len_copy = pltpu.make_async_copy(len_hbm, len_ref, small_sem.at[0])
    order_copy = pltpu.make_async_copy(order_hbm, order_ref, small_sem.at[1])
    len_copy.start()
    order_copy.start()

    z, x = lax.div(me, cols_x), lax.rem(me, cols_x)
    refs = (k_ref, v_ref)

    def block(row, col):
        return pl.ds((row * cols_x + col) * rows, rows)

    def wrapped(row):
        return lax.rem(row + rows_z, rows_z)

    def peer(e):
        return z * cols_x + lax.rem(x + e, cols_x)

    def copy(u, at, target, send, recv):
        return pltpu.make_async_remote_copy(
            src_ref=refs[u].at[at],
            dst_ref=refs[u].at[at],
            send_sem=send,
            recv_sem=recv,
            device_id={"blk": target},
            device_id_type=MESH,
        )

    def to_column(row, u):
        return copy(u, own, row * cols_x + x, col_send.at[row, u], col_recv.at[z, u])

    def from_column(row, u):
        return copy(u, block(row, x), row * cols_x + x, col_send.at[row, u], col_recv.at[row, u])

    def to_row(row, e, u):
        return copy(u, block(row, x), peer(e), row_send.at[row, e - 1, u], row_recv.at[row, e - 1, u])

    def from_row(row, e, u):
        col = lax.rem(x + cols_x - e, cols_x)
        return copy(u, block(row, col), peer(e), row_send.at[row, e - 1, u], row_recv.at[row, e - 1, u])

    def each_row(distances, visit):
        for d in distances:
            pl.when(z + d < rows_z)(lambda d=d: visit(z + d))
            pl.when(z >= d)(lambda d=d: visit(z - d))

    near = range(1, rows_z)
    send_order = tuple(reversed(near))
    barrier = pltpu.get_barrier_semaphore()

    def greet(target):
        pl.semaphore_signal(barrier, inc=1, device_id={"blk": target}, device_id_type=MESH)

    for d in near:
        greet(lax.rem(me + d * cols_x, blocks))
    for e in range(1, cols_x):
        greet(peer(e))
    pl.semaphore_wait(barrier, rows_z + cols_x - 2)

    for u, own_copy in enumerate((k_copy, v_copy)):
        own_copy.wait()
        each_row(send_order, lambda row, u=u: to_column(row, u).start())
        for e in range(1, cols_x):
            to_row(z, e, u).start()

    def relay(row, u):
        from_column(row, u).wait_recv()
        for e in range(1, cols_x):
            to_row(row, e, u).start()

    def gather_row(row, u):
        for e in range(1, cols_x):
            from_row(row, e, u).wait_recv()

    def drain():
        for u in range(2):
            for d in near:
                to_column(lax.rem(z + d, rows_z), u).wait_send()
            for row in range(rows_z):
                for e in range(1, cols_x):
                    to_row(row, e, u).wait_send()

    len_copy.wait()
    order_copy.wait()
    limit = len_ref[0]
    row = lax.broadcasted_iota(jnp.int32, (rows, 1), 0)
    row_pos = jnp.zeros((rows, 1), jnp.int32)
    for t in range(spans):
        row_pos = jnp.where(row // span == t, order_ref[me * spans + t] * span + row % span, row_pos)
    chunk = min(keys, KEY_CHUNK)
    chunks = keys // chunk
    lane = lax.broadcasted_iota(jnp.int32, (1, chunk), 1)

    def make_bias(c):
        key_pos = jnp.zeros((1, chunk), jnp.int32)
        for t in range(chunk // span):
            key_pos = jnp.where(
                lane // span == t, order_ref[c * (chunk // span) + t] * span + lane % span, key_pos
            )
        allowed = (key_pos <= row_pos) & (key_pos < limit)
        bias_ref[c] = jnp.where(allowed, 0.0, NEG_FILL)

    pl.loop(0, chunks)(make_bias)
    live = row_pos < limit
    q_copy.wait()

    for u in range(2):
        each_row(tuple(reversed(near)), lambda row, u=u: relay(row, u))
    for u in range(2):
        for row in range(rows_z):
            gather_row(row, u)

    scale = HEAD_WIDTH ** (-0.5) * math.log2(math.e)
    tile = HEADS_PER_TILE if group % HEADS_PER_TILE == 0 else 1
    height = tile * rows
    ones = jnp.ones((chunk, HEAD_WIDTH), jnp.bfloat16)

    def out_copy(h, p):
        wide = group * HEAD_WIDTH // OUT_PARTS
        at = pl.ds((h * OUT_PARTS + p) * wide, wide)
        return pltpu.make_async_copy(o_ref.at[:, at], o_hbm.at[0, :, at], out_sem.at[h, p])

    for h in range(local_heads):
        cols = slice(h * HEAD_WIDTH, (h + 1) * HEAD_WIDTH)

        def run_tile(i, h=h, cols=cols):
            first = h * group * HEAD_WIDTH + i * (tile * HEAD_WIDTH)

            def q_cols(t):
                return pl.ds(pl.multiple_of(first + t * HEAD_WIDTH, HEAD_WIDTH), HEAD_WIDTH)

            q = jnp.concatenate([q_ref[:, q_cols(t)] for t in range(tile)], axis=0)

            def part(c):
                at = pl.ds(pl.multiple_of(c * chunk, chunk), chunk)
                score = lax.dot_general(
                    q, k_ref[at, cols], (((1,), (1,)), ((), ())), preferred_element_type=jnp.float32
                )
                score = (score * scale).reshape(tile, rows, chunk) + bias_ref[c][None]
                return score.reshape(height, chunk), jnp.concatenate([v_ref[at, cols], ones], axis=1)

            if chunks == 1:
                score, value = part(0)
                top = jnp.max(score, axis=1, keepdims=True)
                weight = jnp.exp2(score - top).astype(jnp.bfloat16)
                mixed = jnp.dot(weight, value, preferred_element_type=jnp.float32)
            else:

                def step(c, state):
                    best, mixed = state
                    score, value = part(c)
                    top = jnp.maximum(best, jnp.max(score, axis=1, keepdims=True))
                    weight = jnp.exp2(score - top).astype(jnp.bfloat16)
                    fresh = jnp.dot(weight, value, preferred_element_type=jnp.float32)
                    return top, mixed * jnp.exp2(best - top) + fresh

                init = (
                    jnp.full((height, 1), NEG_FILL, jnp.float32),
                    jnp.zeros((height, 2 * HEAD_WIDTH), jnp.float32),
                )
                _, mixed = lax.fori_loop(0, chunks, step, init)
            out = mixed[:, :HEAD_WIDTH] / mixed[:, HEAD_WIDTH:]
            for t in range(tile):
                piece = jnp.where(live, out[t * rows : (t + 1) * rows], 0.0)
                o_ref[:, q_cols(t)] = piece.astype(o_ref.dtype)

        tiles = group // tile
        per_part = tiles // OUT_PARTS
        for p in range(OUT_PARTS):
            pl.loop(p * per_part, (p + 1) * per_part, unroll=True)(run_tile)
            out_copy(h, p).start()

    drain()
    for h in range(local_heads):
        for p in range(OUT_PARTS):
            out_copy(h, p).wait()


def solution(mesh):
    blocks = mesh.shape["blk"]
    cols_x = row_length(blocks)
    rows_z = blocks // cols_x

    def shards(queries, keys, values, prompt_length, span_order):
        _, rows, width = queries.shape
        kv_width = keys.shape[2]
        local_heads = kv_width // HEAD_WIDTH
        group = width // kv_width
        total = blocks * rows
        chunk = min(total, KEY_CHUNK)
        anywhere = pl.BlockSpec(memory_space=pltpu.HBM)
        return pl.pallas_call(
            functools.partial(kernel, rows_z, cols_x, local_heads, group, span_order.shape[0] // blocks),
            out_shape=jax.ShapeDtypeStruct(queries.shape, queries.dtype),
            in_specs=[anywhere] * 5,
            out_specs=anywhere,
            scratch_shapes=[
                *[pltpu.VMEM((rows, width), queries.dtype)] * 2,
                pltpu.VMEM((total, kv_width), keys.dtype),
                pltpu.VMEM((total, kv_width), values.dtype),
                pltpu.VMEM((total // chunk, rows, chunk), jnp.float32),
                pltpu.SMEM(prompt_length.shape, jnp.int32),
                pltpu.SMEM(span_order.shape, jnp.int32),
                pltpu.SemaphoreType.DMA,
                pltpu.SemaphoreType.DMA((2,)),
                pltpu.SemaphoreType.DMA((2,)),
                pltpu.SemaphoreType.DMA((local_heads, OUT_PARTS)),
                *[pltpu.SemaphoreType.DMA((rows_z, 2))] * 2,
                *[pltpu.SemaphoreType.DMA((rows_z, cols_x, 2))] * 2,
            ],
            compiler_params=pltpu.CompilerParams(
                collective_id=0, has_side_effects=True, vmem_limit_bytes=VMEM_LIMIT
            ),
        )(queries, keys, values, prompt_length, span_order)

    spec = P("rep", "blk", "head")
    return jax.shard_map(
        shards, mesh=mesh, in_specs=(spec, spec, spec, P("rep"), P("rep")), out_specs=spec, check_vma=False
    )
```

```python
import functools
import math

import jax
import jax.numpy as jnp
from jax import lax
from jax.experimental import pallas as pl
from jax.experimental.pallas import tpu as pltpu
from jax.sharding import PartitionSpec as P

HEAD_WIDTH = 128
NEG_FILL = -1e30
HEADS_PER_TILE = 2
KEY_CHUNK = 512
OUT_PARTS = 2
VMEM_LIMIT = 56 * 1024 * 1024
MESH = pl.DeviceIdType.MESH


def row_length(blocks):
    return max(d for d in range(1, math.isqrt(blocks) + 1) if blocks % d == 0)


def kernel(
    rows_z, cols_x, local_heads, group, spans, q_hbm, k_hbm, v_hbm, len_hbm, order_hbm, o_hbm,
    q_ref, o_ref, k_ref, v_ref, bias_ref, w_ref, len_ref, order_ref, q_sem, own_sem, small_sem, out_sem,
    col_send, col_recv, row_send, row_recv
):
    blocks = rows_z * cols_x
    rows = q_ref.shape[0]
    span = rows // spans
    keys = blocks * rows
    me = lax.axis_index("blk")
    own = pl.ds(me * rows, rows)
    q_copy = pltpu.make_async_copy(q_hbm.at[0], q_ref, q_sem)
    k_copy = pltpu.make_async_copy(k_hbm.at[0], k_ref.at[own], own_sem.at[0])
    v_copy = pltpu.make_async_copy(v_hbm.at[0], v_ref.at[own], own_sem.at[1])
    k_copy.start()
    v_copy.start()
    q_copy.start()
    len_copy = pltpu.make_async_copy(len_hbm, len_ref, small_sem.at[0])
    order_copy = pltpu.make_async_copy(order_hbm, order_ref, small_sem.at[1])
    len_copy.start()
    order_copy.start()

    z, x = lax.div(me, cols_x), lax.rem(me, cols_x)
    refs = (k_ref, v_ref)

    def block(row, col):
        return pl.ds((row * cols_x + col) * rows, rows)

    def wrapped(row):
        return lax.rem(row + rows_z, rows_z)

    def peer(e):
        return z * cols_x + lax.rem(x + e, cols_x)

    def copy(u, at, target, send, recv):
        return pltpu.make_async_remote_copy(
            src_ref=refs[u].at[at],
            dst_ref=refs[u].at[at],
            send_sem=send,
            recv_sem=recv,
            device_id={"blk": target},
            device_id_type=MESH,
        )

    def to_column(row, u):
        return copy(u, own, row * cols_x + x, col_send.at[row, u], col_recv.at[z, u])

    def from_column(row, u):
        return copy(u, block(row, x), row * cols_x + x, col_send.at[row, u], col_recv.at[row, u])

    def to_row(row, e, u):
        return copy(u, block(row, x), peer(e), row_send.at[row, e - 1, u], row_recv.at[row, e - 1, u])

    def from_row(row, e, u):
        col = lax.rem(x + cols_x - e, cols_x)
        return copy(u, block(row, col), peer(e), row_send.at[row, e - 1, u], row_recv.at[row, e - 1, u])

    def each_row(distances, visit):
        for d in distances:
            pl.when(z + d < rows_z)(lambda d=d: visit(z + d))
            pl.when(z >= d)(lambda d=d: visit(z - d))

    near = range(1, rows_z)
    send_order = tuple(reversed(near))
    barrier = pltpu.get_barrier_semaphore()

    def greet(target):
        pl.semaphore_signal(barrier, inc=1, device_id={"blk": target}, device_id_type=MESH)

    for d in near:
        greet(lax.rem(me + d * cols_x, blocks))
    for e in range(1, cols_x):
        greet(peer(e))
    pl.semaphore_wait(barrier, rows_z + cols_x - 2)

    for u, own_copy in enumerate((k_copy, v_copy)):
        own_copy.wait()
        each_row(send_order, lambda row, u=u: to_column(row, u).start())
        for e in range(1, cols_x):
            to_row(z, e, u).start()

    def relay(row, u):
        from_column(row, u).wait_recv()
        for e in range(1, cols_x):
            to_row(row, e, u).start()

    def gather_row(row, u):
        for e in range(1, cols_x):
            from_row(row, e, u).wait_recv()

    def drain():
        for u in range(2):
            for d in near:
                to_column(lax.rem(z + d, rows_z), u).wait_send()
            for row in range(rows_z):
                for e in range(1, cols_x):
                    to_row(row, e, u).wait_send()

    len_copy.wait()
    order_copy.wait()
    limit = len_ref[0]
    row = lax.broadcasted_iota(jnp.int32, (rows, 1), 0)
    row_pos = jnp.zeros((rows, 1), jnp.int32)
    for t in range(spans):
        row_pos = jnp.where(row // span == t, order_ref[me * spans + t] * span + row % span, row_pos)
    chunk = min(keys, KEY_CHUNK)
    chunks = keys // chunk
    lane = lax.broadcasted_iota(jnp.int32, (1, chunk), 1)

    def make_bias(c):
        key_pos = jnp.zeros((1, chunk), jnp.int32)
        for t in range(chunk // span):
            key_pos = jnp.where(
                lane // span == t, order_ref[c * (chunk // span) + t] * span + lane % span, key_pos
            )
        allowed = (key_pos <= row_pos) & (key_pos < limit)
        bias_ref[c] = jnp.where(allowed, 0.0, NEG_FILL)

    pl.loop(0, chunks)(make_bias)
    live = row_pos < limit
    q_copy.wait()

    for u in range(2):
        each_row(tuple(reversed(near)), lambda row, u=u: relay(row, u))
    for row in range(rows_z):
        gather_row(row, 0)

    def gather_values():
        for row in range(rows_z):
            gather_row(row, 1)

    scale = HEAD_WIDTH ** (-0.5) * math.log2(math.e)
    tile = HEADS_PER_TILE if group % HEADS_PER_TILE == 0 else 1
    height = tile * rows
    ones = jnp.ones((chunk, HEAD_WIDTH), jnp.bfloat16)

    def out_copy(h, p):
        wide = group * HEAD_WIDTH // OUT_PARTS
        at = pl.ds((h * OUT_PARTS + p) * wide, wide)
        return pltpu.make_async_copy(o_ref.at[:, at], o_hbm.at[0, :, at], out_sem.at[h, p])

    if chunks > 1:
        gather_values()

    for phase, h in [(p, h) for p in range(2 if chunks == 1 else 1) for h in range(local_heads)]:
        if phase == 1 and h == 0:
            gather_values()
        cols = slice(h * HEAD_WIDTH, (h + 1) * HEAD_WIDTH)

        def run_tile(i, h=h, cols=cols, phase=phase):
            first = h * group * HEAD_WIDTH + i * (tile * HEAD_WIDTH)

            def q_cols(t):
                return pl.ds(pl.multiple_of(first + t * HEAD_WIDTH, HEAD_WIDTH), HEAD_WIDTH)

            kept = pl.ds(pl.multiple_of((h * (group // tile) + i) * height, height), height)
            q = jnp.concatenate([q_ref[:, q_cols(t)] for t in range(tile)], axis=0)

            def score_of(c):
                at = pl.ds(pl.multiple_of(c * chunk, chunk), chunk)
                score = lax.dot_general(
                    q, k_ref[at, cols], (((1,), (1,)), ((), ())), preferred_element_type=jnp.float32
                )
                score = (score * scale).reshape(tile, rows, chunk) + bias_ref[c][None]
                return score.reshape(height, chunk)

            def value_of(c):
                at = pl.ds(pl.multiple_of(c * chunk, chunk), chunk)
                return jnp.concatenate([v_ref[at, cols], ones], axis=1)

            if chunks == 1 and phase == 0:
                score = score_of(0)
                top = jnp.max(score, axis=1, keepdims=True)
                w_ref[kept] = jnp.exp2(score - top).astype(jnp.bfloat16)
                return
            if chunks == 1:
                mixed = jnp.dot(w_ref[kept], value_of(0), preferred_element_type=jnp.float32)
            else:

                def step(c, state):
                    best, mixed = state
                    score, value = score_of(c), value_of(c)
                    top = jnp.maximum(best, jnp.max(score, axis=1, keepdims=True))
                    weight = jnp.exp2(score - top).astype(jnp.bfloat16)
                    fresh = jnp.dot(weight, value, preferred_element_type=jnp.float32)
                    return top, mixed * jnp.exp2(best - top) + fresh

                init = (
                    jnp.full((height, 1), NEG_FILL, jnp.float32),
                    jnp.zeros((height, 2 * HEAD_WIDTH), jnp.float32),
                )
                _, mixed = lax.fori_loop(0, chunks, step, init)
            out = mixed[:, :HEAD_WIDTH] / mixed[:, HEAD_WIDTH:]
            for t in range(tile):
                piece = jnp.where(live, out[t * rows : (t + 1) * rows], 0.0)
                o_ref[:, q_cols(t)] = piece.astype(o_ref.dtype)

        tiles = group // tile
        per_part = tiles // OUT_PARTS
        for p in range(OUT_PARTS):
            pl.loop(p * per_part, (p + 1) * per_part, unroll=True)(run_tile)
            if phase == 1 or chunks > 1:
                out_copy(h, p).start()

    drain()
    for h in range(local_heads):
        for p in range(OUT_PARTS):
            out_copy(h, p).wait()


def solution(mesh):
    blocks = mesh.shape["blk"]
    cols_x = row_length(blocks)
    rows_z = blocks // cols_x

    def shards(queries, keys, values, prompt_length, span_order):
        _, rows, width = queries.shape
        kv_width = keys.shape[2]
        local_heads = kv_width // HEAD_WIDTH
        group = width // kv_width
        total = blocks * rows
        chunk = min(total, KEY_CHUNK)
        anywhere = pl.BlockSpec(memory_space=pltpu.HBM)
        return pl.pallas_call(
            functools.partial(kernel, rows_z, cols_x, local_heads, group, span_order.shape[0] // blocks),
            out_shape=jax.ShapeDtypeStruct(queries.shape, queries.dtype),
            in_specs=[anywhere] * 5,
            out_specs=anywhere,
            scratch_shapes=[
                *[pltpu.VMEM((rows, width), queries.dtype)] * 2,
                pltpu.VMEM((total, kv_width), keys.dtype),
                pltpu.VMEM((total, kv_width), values.dtype),
                pltpu.VMEM((total // chunk, rows, chunk), jnp.float32),
                pltpu.VMEM((local_heads * group * rows if chunk == total else rows, chunk), jnp.bfloat16),
                pltpu.SMEM(prompt_length.shape, jnp.int32),
                pltpu.SMEM(span_order.shape, jnp.int32),
                pltpu.SemaphoreType.DMA,
                pltpu.SemaphoreType.DMA((2,)),
                pltpu.SemaphoreType.DMA((2,)),
                pltpu.SemaphoreType.DMA((local_heads, OUT_PARTS)),
                *[pltpu.SemaphoreType.DMA((rows_z, 2))] * 2,
                *[pltpu.SemaphoreType.DMA((rows_z, cols_x, 2))] * 2,
            ],
            compiler_params=pltpu.CompilerParams(
                collective_id=0, has_side_effects=True, vmem_limit_bytes=VMEM_LIMIT
            ),
        )(queries, keys, values, prompt_length, span_order)

    spec = P("rep", "blk", "head")
    return jax.shard_map(
        shards, mesh=mesh, in_specs=(spec, spec, spec, P("rep"), P("rep")), out_specs=spec, check_vma=False
    )
```
